256 devices in a mesh: blk: 128 (over x_lo, z, y, core), aux: 2 (over x_hi).
Axes of the slice: x: 4 (x_hi: 2, x_lo: 2; x = x_hi * 2 + x_lo), y: 4, z: 8, core: 2. Of those that a mesh axis runs over, the one named last changes fastest.
Arguments:
- panels: bfloat16 [4, 11264, 120, 120], P(None, ('blk', 'aux')), may hold values from -0.19921875 to 0.19921875
- aux_counts: int32 [256], replicated, may hold values from 1 to 44, 9000 in all
- pair_list: int32 [512, 2], replicated, may hold values from 0 to 3
- pair_ranks: int32 [512], replicated, may hold values from 24 to 120
- amplitudes: bfloat16 [512, 120, 120], P('blk'), may hold values from -6 to 6
Outputs:
- residual: float32 [512, 120, 120], P('blk', 'aux')
The draws below stay inside these ranges and needn't reach their ends.
Inputs may be any that keep to these rules, and one draw needn't show every extreme that they name: `aux_counts`: entry k counts the live auxiliary functions of panel shard k (slots k * 44 onward), which come first in the shard; the entries sum to 9000.
All inputs are finite; a program needn't handle non-finite values.
Results may differ from the reference program's by a relative error of at most 0.0029.
Values may be sent and summed in bfloat16 or wider, within the bound.
No kernel may reach another device: no remote copies, remote signals or barrier semaphores. Data moves between devices by JAX's collectives and lax.ppermute only.
A program may use at most 64 MiB of HBM per device.

```python
import math
import jax
import jax.numpy as jnp
import numpy as np
from jax import lax

R = 120
NAUX = 9000
NOCC = 4
PAIRS_DEV = 4
AUX_SLOT = 44
AUX_ROWS = 11264
PAIRS = 512
N_BLK = 128
N_AUX = 2
DEVICES = 256


def with_ends(values, key, smallest, largest):
    longest = values.shape.index(max(values.shape))
    spots = []
    for shift in (0, 1):
        where = [jax.random.randint(jax.random.fold_in(key, axis), (), 0, length) for axis, length in enumerate(values.shape)]
        where[longest] = (where[longest] + shift) % values.shape[longest]
        spots.append(tuple(where))
    return values.at[spots[0]].set(smallest).at[spots[1]].set(largest)


def block_scale(key, extent, shards, least, high):
    factor_of = 1.0
    for position, shards_of in shards:
        heights = jax.random.uniform(jax.random.fold_in(jax.random.fold_in(key, 6), position), (shards_of,), jnp.float32, least / len(shards), high / len(shards))
        factor_of = factor_of * jnp.repeat(jnp.exp(heights), extent[position] // shards_of).reshape((-1,) + (1,) * (len(extent) - 1 - position))
    return factor_of


def profile(count, total, bound, lean):
    weights = [(1 << 20) // math.isqrt(rank ** lean) + 1 for rank in range(2, count + 1)]
    surplus, given = total - bound - (count - 1), [1] * (count - 1)
    while surplus > 0:
        movable = [i for i in range(count - 1) if given[i] < bound]
        mass, remaining = sum([weights[i] for i in movable]), surplus
        for i in movable:
            addition = min(bound - given[i], max(1, remaining * weights[i] // mass), surplus)
            given[i] = given[i] + addition
            surplus = surplus - addition
    return np.array([bound] + given)


def ragged_sizes(stream_key, amount, total, bound, slope):
    if amount == 2:
        one = jax.random.randint(stream_key, (), max(1, total - bound), min(bound, total - 1) + 1)
        return jnp.stack([one, total - one])
    sizes = jnp.asarray(profile(amount, total, bound, slope), jnp.int32)
    twos = (amount - 1) // 2
    source_of, receiver = sizes[1:1 + 2 * twos:2], sizes[2:2 + 2 * twos:2]
    room = jnp.minimum(source_of - 1, bound - receiver)
    shifted = jax.random.randint(jax.random.fold_in(stream_key, 1), (twos,), 0, 1 << 20) % (room + 1)
    sizes = sizes.at[1:1 + 2 * twos:2].set(source_of - shifted).at[2:2 + 2 * twos:2].set(receiver + shifted)
    return sizes[jax.random.permutation(jax.random.fold_in(stream_key, 2), amount)]


def noise(own_key, dims, spread, reach, split=(), kind=jnp.bfloat16):
    loudness = block_scale(own_key, dims, split, -0.22, 0.18) if split else 1.0
    array = jax.random.normal(own_key, dims, jnp.float32) * spread * loudness
    return jnp.minimum(jnp.maximum(array, -reach), reach).astype(kind)


def setup_inputs(seed: int = 0) -> dict:
    key_of = jax.random.split(jax.random.key(seed), 6)
    panels = noise(key_of[0], (NOCC, AUX_ROWS, R, R), 0.03, 0.19921875, ((1, 256),))
    aux_counts = ragged_sizes(key_of[1], DEVICES, NAUX, AUX_SLOT, 1).astype(jnp.int32)
    pair_list = with_ends(jax.random.randint(key_of[2], (PAIRS, 2), 0, NOCC), jax.random.fold_in(key_of[2], 1), 0, NOCC - 1).astype(jnp.int32)
    pair_ranks = with_ends(jax.random.randint(key_of[3], (PAIRS,), R // 5, R + 1), jax.random.fold_in(key_of[3], 1), R // 5, R).astype(jnp.int32)
    amplitudes = noise(key_of[4], (PAIRS, R, R), 1.0, 6.0, ((0, 128),))
    return dict(panels=panels, aux_counts=aux_counts, pair_list=pair_list, pair_ranks=pair_ranks, amplitudes=amplitudes)


pair_group = 4


def ladder(block, count, pair_rows, rank_rows, amp_rows):
    slot_count = block.shape[1]
    pno_width = block.shape[2]
    live_slots = jnp.arange(slot_count, dtype=jnp.int32) < count
    positions = jnp.arange(pno_width, dtype=jnp.int32)
    group_count = pair_rows.shape[0] // pair_group

    def one_group(group_item):
        group_pairs, group_ranks, group_amps = group_item
        kept_mask = positions[None, :] < group_ranks[:, None]
        pair_mask = kept_mask[:, :, None] & kept_mask[:, None, :]
        masked = jnp.where(pair_mask, group_amps, jnp.zeros_like(group_amps))
        left_panel = jnp.take(block, group_pairs[:, 0], axis=0)
        right_panel = jnp.take(block, group_pairs[:, 1], axis=0)
        half_step = jnp.einsum("gsac,gcd->gsad", left_panel.astype(jnp.float32), masked.astype(jnp.float32))
        half_step = jnp.where(live_slots[None, :, None, None], half_step, jnp.zeros_like(half_step)).astype(jnp.bfloat16)
        ladder_sum = jnp.einsum("gsad,gsbd->gab", half_step.astype(jnp.float32), right_panel.astype(jnp.float32))
        return jnp.where(pair_mask, ladder_sum, jnp.zeros_like(ladder_sum))

    results = lax.map(one_group, (pair_rows.reshape(group_count, pair_group, 2), rank_rows.reshape(group_count, pair_group), amp_rows.reshape(group_count, pair_group, pno_width, pno_width)))
    return results.reshape(pair_rows.shape[0], pno_width, pno_width)


def reference(panels, aux_counts, pair_list, pair_ranks, amplitudes):
    blocked = panels.reshape(NOCC, N_BLK, N_AUX, AUX_SLOT, R, R)
    counts_grid = aux_counts.reshape(N_BLK, N_AUX)
    pairs_grid = pair_list.reshape(N_BLK, PAIRS_DEV, 2)
    ranks_grid = pair_ranks.reshape(N_BLK, PAIRS_DEV)
    amps_grid = amplitudes.reshape(N_BLK, PAIRS_DEV, R, R)

    def owner_sum(owner_index):
        accum = jnp.zeros((PAIRS_DEV, R, R), jnp.float32)
        for offset in range(3):
            source = (owner_index - offset) % N_BLK
            for member in range(N_AUX):
                accum = accum + ladder(blocked[:, source, member], counts_grid[source, member], pairs_grid[owner_index], ranks_grid[owner_index], amps_grid[owner_index])
        return accum

    result = lax.map(owner_sum, jnp.arange(N_BLK, dtype=jnp.int32))
    return result.reshape(N_BLK * PAIRS_DEV, R, R)
```

```python
import functools
import jax
import jax.numpy as jnp
from jax import lax
from jax.experimental import pallas as pl
from jax.experimental.pallas import tpu as pltpu
from jax.sharding import PartitionSpec as P

F32, BF16 = jnp.float32, jnp.bfloat16
SLAB = 128
WIDE = 256
STEP = 2


def meta_copies(counts, pairs, ranks, counts_s, pairs_s, ranks_s, sems):
    return [
        pltpu.make_async_copy(counts, counts_s, sems.at[0]),
        pltpu.make_async_copy(pairs, pairs_s, sems.at[1]),
        pltpu.make_async_copy(ranks, ranks_s, sems.at[2]),
    ]


def one_pair(row, amps, put, paired, both, pairs_s, ranks_s, width):
    left, right, rank = pairs_s[0, row], pairs_s[1, row], ranks_s[row]
    rows = lax.broadcasted_iota(jnp.int32, (width, width), 0)
    cols = lax.broadcasted_iota(jnp.int32, (width, width), 1)
    keep = (rows < rank) & (cols < rank)
    masked = jnp.where(keep, amps, jnp.zeros_like(amps))
    both[0:width, 0:width] = masked
    both[SLAB : SLAB + width, SLAB : SLAB + width] = masked
    total = jnp.zeros((SLAB, SLAB), F32)
    slot_pairs = paired.shape[1]
    for first in range(0, slot_pairs, STEP):
        taken = min(STEP, slot_pairs - first)
        lhs = paired[left, first : first + taken].reshape(taken * SLAB, WIDE)
        half = jnp.dot(lhs, both[...], preferred_element_type=F32)
        for k in range(taken):
            part = half[k * SLAB : (k + 1) * SLAB].astype(BF16)
            total = total + lax.dot_general(
                part, paired[right, first + k], (((1,), (1,)), ((), ())), preferred_element_type=F32
            )
    put(jnp.where(keep, total[:width, :width], 0.0))


def own_body(counts, pairs, ranks, amps, panels, out, paired, raw, both, counts_s, pairs_s, ranks_s, sems, meta_sems):
    orbitals, slots, width, _ = panels.shape
    owned = amps.shape[0]
    cut = width // 2
    block = lax.axis_index("blk")
    shard = block * lax.axis_size("aux") + lax.axis_index("aux")
    copies = [pltpu.make_async_copy(panels.at[o], raw.at[o], sems.at[o]) for o in range(orbitals)]
    for copy in copies:
        copy.start()
    small = meta_copies(counts, pairs, ranks, counts_s, pairs_s, ranks_s, meta_sems)
    for copy in small:
        copy.start()
    both[...] = jnp.zeros_like(both)
    for copy in small:
        copy.wait()
    live = counts_s[shard]
    for o in range(orbitals):
        copies[o].wait()

        def widen(t, carry):
            for side in range(2):
                slot = 2 * t + side
                slab = raw[o, slot]
                slab = jnp.where(slot < live, slab, jnp.zeros_like(slab))
                slab = jnp.pad(slab, ((0, SLAB - width), (0, SLAB - width)))
                paired[o, t, :, side * SLAB : (side + 1) * SLAB] = slab
            return carry

        lax.fori_loop(0, slots // 2, widen, 0, unroll=2)

    def pair(p, carry):
        def put(value):
            out[0, p] = value[:cut]
            out[1, p] = value[cut:]

        one_pair(block * owned + p, amps[p], put, paired, both, pairs_s, ranks_s, width)
        return carry

    lax.fori_loop(0, owned, pair, 0)


def other_body(pairs, ranks, near, far, paired, near_out, far_out, both, pairs_s, ranks_s, meta_sems):
    owned, width, _ = near.shape
    cut = width // 2
    blocks = lax.axis_size("blk")
    block = lax.axis_index("blk")
    small = [
        pltpu.make_async_copy(pairs, pairs_s, meta_sems.at[0]),
        pltpu.make_async_copy(ranks, ranks_s, meta_sems.at[1]),
    ]
    for copy in small:
        copy.start()
    both[...] = jnp.zeros_like(both)
    for copy in small:
        copy.wait()
    for amps, out, hops in ((far, far_out, 2), (near, near_out, 1)):
        start = (block + hops) % blocks * owned

        def pair(p, carry):
            def put(value):
                out[0, p] = value[:cut].astype(BF16)
                out[1, p] = value[cut:].astype(BF16)

            one_pair(start + p, amps[p], put, paired, both, pairs_s, ranks_s, width)
            return carry

        lax.fori_loop(0, owned, pair, 0)


def in_vmem():
    return pl.BlockSpec(memory_space=pltpu.VMEM)


def in_place():
    return pl.BlockSpec(memory_space=pltpu.HBM)


def kept_in_hbm(value):
    return pltpu.with_memory_space_constraint(value, pltpu.HBM)


def own_terms(counts, pairs, ranks, amps, panels):
    owned, width, _ = amps.shape
    orbitals, slots, _, _ = panels.shape
    paired = (orbitals, slots // 2, SLAB, WIDE)
    return pl.pallas_call(
        own_body,
        out_shape=(
            jax.ShapeDtypeStruct((2, owned, width // 2, width), F32),
            pltpu.VMEM(paired, BF16),
        ),
        in_specs=[in_place(), in_place(), in_place(), in_vmem(), in_place()],
        out_specs=(in_vmem(), in_vmem()),
        scratch_shapes=[
            pltpu.VMEM(panels.shape, BF16),
            pltpu.VMEM((WIDE, WIDE), BF16),
            pltpu.SMEM(counts.shape, jnp.int32),
            pltpu.SMEM(pairs.shape, jnp.int32),
            pltpu.SMEM(ranks.shape, jnp.int32),
            pltpu.SemaphoreType.DMA((orbitals,)),
            pltpu.SemaphoreType.DMA((3,)),
        ],
        cost_estimate=pl.CostEstimate(flops=4 * 10**9, bytes_accessed=5 * 10**6, transcendentals=0),
        compiler_params=pltpu.CompilerParams(vmem_limit_bytes=16 * 2**20),
        name="own_terms",
    )(counts, pairs, ranks, amps, panels)


def other_terms(pairs, ranks, near, far, paired):
    owned, width, _ = near.shape
    shape = jax.ShapeDtypeStruct((2, owned, width // 2, width), BF16)
    return pl.pallas_call(
        other_body,
        out_shape=(shape, shape),
        in_specs=[in_place(), in_place(), in_vmem(), in_vmem(), in_vmem()],
        out_specs=(in_vmem(), in_vmem()),
        scratch_shapes=[
            pltpu.VMEM((WIDE, WIDE), BF16),
            pltpu.SMEM(pairs.shape, jnp.int32),
            pltpu.SMEM(ranks.shape, jnp.int32),
            pltpu.SemaphoreType.DMA((2,)),
        ],
        cost_estimate=pl.CostEstimate(flops=8 * 10**9, bytes_accessed=5 * 10**6, transcendentals=0),
        compiler_params=pltpu.CompilerParams(vmem_limit_bytes=16 * 2**20),
        name="other_terms",
    )(pairs, ranks, near, far, paired)


def passed_along(value, axis, steps):
    count = lax.axis_size(axis)
    return lax.ppermute(value, axis, [(source, (source + steps) % count) for source in range(count)])


def shards(panels, aux_counts, pair_list, pair_ranks, amplitudes):
    side = lax.axis_index("aux")
    panels = kept_in_hbm(panels)
    pairs = kept_in_hbm(pair_list.T)
    pair_ranks = kept_in_hbm(pair_ranks)
    aux_counts = kept_in_hbm(aux_counts)
    far_amps = passed_along(amplitudes, "blk", -2)
    near_amps = passed_along(amplitudes, "blk", -1)
    own, paired = own_terms(aux_counts, pairs, pair_ranks, amplitudes, panels)
    near, far = other_terms(pairs, pair_ranks, near_amps, far_amps, paired)
    far = passed_along(far, "blk", 2)
    near = passed_along(near, "blk", 1)

    def summed(which):
        parts = [lax.dynamic_index_in_dim(x, which, 0, keepdims=False).astype(F32) for x in (own, near, far)]
        return parts[0] + parts[1] + parts[2]

    received = passed_along(summed(1 - side).astype(BF16), "aux", 1)
    return summed(side) + received.astype(F32)


def solution(mesh):
    placed = (P(None, ("blk", "aux"), None, None), P(), P(), P(), P("blk", None, None))
    return jax.shard_map(
        shards, mesh=mesh, in_specs=placed, out_specs=P("blk", "aux", None), check_vma=False
    )
```

```python
import functools
import jax
import jax.numpy as jnp
from jax import lax
from jax.experimental import pallas as pl
from jax.experimental.pallas import tpu as pltpu
from jax.sharding import PartitionSpec as P

F32, BF16 = jnp.float32, jnp.bfloat16
SLAB = 128
WIDE = 256
STEP = 2


def table_copies(pairs, ranks, pairs_s, ranks_s, sems):
    return [
        pltpu.make_async_copy(pairs, pairs_s, sems.at[0]),
        pltpu.make_async_copy(ranks, ranks_s, sems.at[1]),
    ]


def one_pair(row, amps, put, paired, both, pairs_s, ranks_s, width):
    left, right, rank = pairs_s[0, row], pairs_s[1, row], ranks_s[row]
    rows = lax.broadcasted_iota(jnp.int32, (width, width), 0)
    cols = lax.broadcasted_iota(jnp.int32, (width, width), 1)
    keep = (rows < rank) & (cols < rank)
    masked = jnp.where(keep, amps, jnp.zeros_like(amps))
    both[0:width, 0:width] = masked
    both[SLAB : SLAB + width, SLAB : SLAB + width] = masked
    total = jnp.zeros((SLAB, SLAB), F32)
    slot_pairs = paired.shape[1]
    for first in range(0, slot_pairs, STEP):
        taken = min(STEP, slot_pairs - first)
        lhs = paired[left, first : first + taken].reshape(taken * SLAB, WIDE)
        half = jnp.dot(lhs, both[...], preferred_element_type=F32)
        for k in range(taken):
            part = half[k * SLAB : (k + 1) * SLAB].astype(BF16)
            total = total + lax.dot_general(
                part, paired[right, first + k], (((1,), (1,)), ((), ())), preferred_element_type=F32
            )
    put(jnp.where(keep, total[:width, :width], 0.0))


def load_body(counts, panels, paired, raw, counts_s, sems, count_sem):
    orbitals, slots, width, _ = panels.shape
    shard = lax.axis_index("blk") * lax.axis_size("aux") + lax.axis_index("aux")
    copies = [pltpu.make_async_copy(panels.at[o], raw.at[o], sems.at[o]) for o in range(orbitals)]
    small = pltpu.make_async_copy(counts, counts_s, count_sem)
    small.start()
    for copy in copies:
        copy.start()
    small.wait()
    live = counts_s[shard]
    for o in range(orbitals):
        copies[o].wait()

        def widen(t, carry):
            for side in range(2):
                slot = 2 * t + side
                slab = raw[o, slot]
                slab = jnp.where(slot < live, slab, jnp.zeros_like(slab))
                slab = jnp.pad(slab, ((0, SLAB - width), (0, SLAB - width)))
                paired[o, t, :, side * SLAB : (side + 1) * SLAB] = slab
            return carry

        lax.fori_loop(0, slots // 2, widen, 0, unroll=2)


def group(first, amps, out, paired, both, pairs_s, ranks_s):
    owned, width, _ = amps.shape
    cut = width // 2

    def pair(p, carry):
        def put(value):
            out[0, p] = value[:cut].astype(out.dtype)
            out[1, p] = value[cut:].astype(out.dtype)

        one_pair(first + p, amps[p], put, paired, both, pairs_s, ranks_s, width)
        return carry

    lax.fori_loop(0, owned, pair, 0)


def own_body(pairs, ranks, amps, paired, after, out, both, pairs_s, ranks_s, sems):
    del after
    small = table_copies(pairs, ranks, pairs_s, ranks_s, sems)
    for copy in small:
        copy.start()
    both[...] = jnp.zeros_like(both)
    for copy in small:
        copy.wait()
    group(lax.axis_index("blk") * amps.shape[0], amps, out, paired, both, pairs_s, ranks_s)


def other_body(pairs, ranks, near, far, paired, near_out, far_out, both, pairs_s, ranks_s, sems):
    owned = near.shape[0]
    blocks = lax.axis_size("blk")
    block = lax.axis_index("blk")
    small = table_copies(pairs, ranks, pairs_s, ranks_s, sems)
    for copy in small:
        copy.start()
    both[...] = jnp.zeros_like(both)
    for copy in small:
        copy.wait()
    for amps, out, hops in ((far, far_out, 2), (near, near_out, 1)):
        group((block + hops) % blocks * owned, amps, out, paired, both, pairs_s, ranks_s)


def in_vmem():
    return pl.BlockSpec(memory_space=pltpu.VMEM)


def in_place():
    return pl.BlockSpec(memory_space=pltpu.HBM)


def kept_in_hbm(value):
    return pltpu.with_memory_space_constraint(value, pltpu.HBM)


def loaded(counts, panels):
    orbitals, slots, _, _ = panels.shape
    return pl.pallas_call(
        load_body,
        out_shape=pltpu.VMEM((orbitals, slots // 2, SLAB, WIDE), BF16),
        in_specs=[in_place(), in_place()],
        out_specs=in_vmem(),
        scratch_shapes=[
            pltpu.VMEM(panels.shape, BF16),
            pltpu.SMEM(counts.shape, jnp.int32),
            pltpu.SemaphoreType.DMA((orbitals,)),
            pltpu.SemaphoreType.DMA(()),
        ],
        cost_estimate=pl.CostEstimate(flops=10**9, bytes_accessed=5 * 10**6, transcendentals=0),
        compiler_params=pltpu.CompilerParams(vmem_limit_bytes=16 * 2**20),
        name="loaded",
    )(counts, panels)


def table_scratch(pairs, ranks):
    return [
        pltpu.VMEM((WIDE, WIDE), BF16),
        pltpu.SMEM(pairs.shape, jnp.int32),
        pltpu.SMEM(ranks.shape, jnp.int32),
        pltpu.SemaphoreType.DMA((2,)),
    ]


def own_terms(pairs, ranks, amps, paired, after):
    owned, width, _ = amps.shape
    return pl.pallas_call(
        own_body,
        out_shape=jax.ShapeDtypeStruct((2, owned, width // 2, width), F32),
        in_specs=[in_place(), in_place(), in_vmem(), in_vmem(), pl.BlockSpec(memory_space=pl.ANY)],
        out_specs=in_vmem(),
        scratch_shapes=table_scratch(pairs, ranks),
        cost_estimate=pl.CostEstimate(flops=4 * 10**9, bytes_accessed=5 * 10**6, transcendentals=0),
        compiler_params=pltpu.CompilerParams(vmem_limit_bytes=8 * 2**20),
        name="own_terms",
    )(pairs, ranks, amps, paired, after)


def other_terms(pairs, ranks, near, far, paired):
    owned, width, _ = near.shape
    shape = jax.ShapeDtypeStruct((2, owned, width // 2, width), BF16)
    return pl.pallas_call(
        other_body,
        out_shape=(shape, shape),
        in_specs=[in_place(), in_place(), in_vmem(), in_vmem(), in_vmem()],
        out_specs=(in_vmem(), in_vmem()),
        scratch_shapes=table_scratch(pairs, ranks),
        cost_estimate=pl.CostEstimate(flops=8 * 10**9, bytes_accessed=5 * 10**6, transcendentals=0),
        compiler_params=pltpu.CompilerParams(vmem_limit_bytes=8 * 2**20),
        name="other_terms",
    )(pairs, ranks, near, far, paired)


def passed_along(value, axis, steps):
    count = lax.axis_size(axis)
    return lax.ppermute(value, axis, [(source, (source + steps) % count) for source in range(count)])


def shards(panels, aux_counts, pair_list, pair_ranks, amplitudes):
    side = lax.axis_index("aux")
    pairs = kept_in_hbm(pair_list.T)
    ranks = kept_in_hbm(pair_ranks)
    far_amps = passed_along(amplitudes, "blk", -2)
    near_amps = passed_along(amplitudes, "blk", -1)
    paired = loaded(kept_in_hbm(aux_counts), kept_in_hbm(panels))
    near, far = other_terms(pairs, ranks, near_amps, far_amps, paired)
    own = own_terms(pairs, ranks, amplitudes, paired, far)
    far = passed_along(far, "blk", 2)
    near = passed_along(near, "blk", 1)

    def summed(which):
        parts = [lax.dynamic_index_in_dim(x, which, 0, keepdims=False).astype(F32) for x in (own, near, far)]
        return parts[0] + parts[1] + parts[2]

    received = passed_along(summed(1 - side).astype(BF16), "aux", 1)
    return summed(side) + received.astype(F32)


def solution(mesh):
    placed = (P(None, ("blk", "aux"), None, None), P(), P(), P(), P("blk", None, None))
    return jax.shard_map(
        shards, mesh=mesh, in_specs=placed, out_specs=P("blk", "aux", None), check_vma=False
    )
```

```python
import jax
import jax.numpy as jnp
from jax import lax
from jax.experimental import pallas as pl
from jax.experimental.pallas import tpu as pltpu
from jax.sharding import PartitionSpec as P

F32, BF16 = jnp.float32, jnp.bfloat16
SLAB = 128
STEP = 2
EARLY = 2


def table_copies(pairs, ranks, pairs_s, ranks_s, sems):
    return [
        pltpu.make_async_copy(pairs, pairs_s, sems.at[0]),
        pltpu.make_async_copy(ranks, ranks_s, sems.at[1]),
    ]


def slot_pair(paired, orbital, t):
    return jnp.concatenate([paired[orbital, t, 0], paired[orbital, t, 1]], axis=1)


def on_diagonal(square):
    empty = jnp.zeros_like(square)
    upper = jnp.concatenate([square, empty], axis=1)
    lower = jnp.concatenate([empty, square], axis=1)
    return jnp.concatenate([upper, lower], axis=0)


def terms(work, paired, squares, pairs_s, ranks_s):
    slot_pairs = paired.shape[1]
    prepared = []
    for n, (row, amps, put) in enumerate(work):
        width = amps.shape[0]
        rank = ranks_s[row]
        rows = lax.broadcasted_iota(jnp.int32, (width, width), 0)
        cols = lax.broadcasted_iota(jnp.int32, (width, width), 1)
        masked = jnp.where((rows < rank) & (cols < rank), amps, jnp.zeros_like(amps))
        squares[n] = jnp.pad(masked, ((0, SLAB - width), (0, SLAB - width)))
        prepared.append((pairs_s[0, row], pairs_s[1, row], rank, rows, cols, put))
    for n, (left, right, rank, rows, cols, put) in enumerate(prepared):
        width = rows.shape[0]
        total = jnp.zeros((SLAB, SLAB), F32)
        for first in range(0, slot_pairs, STEP):
            taken = range(first, min(first + STEP, slot_pairs))
            lhs = jnp.concatenate([slot_pair(paired, left, t) for t in taken], axis=0)
            half = jnp.dot(lhs, on_diagonal(squares[n]), preferred_element_type=F32)
            for k, t in enumerate(taken):
                part = half[k * SLAB : (k + 1) * SLAB].astype(BF16)
                total = total + lax.dot_general(
                    part, slot_pair(paired, right, t), (((1,), (1,)), ((), ())), preferred_element_type=F32
                )
        put(jnp.where((rows < rank) & (cols < rank), total[:width, :width], 0.0))


def stored(out, p):
    def put(value):
        cut = value.shape[0] // 2
        out[0, p] = value[:cut].astype(out.dtype)
        out[1, p] = value[cut:].astype(out.dtype)

    return put


def load_body(counts, pairs, ranks, amps, panels, paired, out, raw, amps_v, squares, counts_s, pairs_s, ranks_s, sems, small_sems):
    orbitals, slots, width, _ = panels.shape
    owned = amps.shape[0]
    block = lax.axis_index("blk")
    shard = block * lax.axis_size("aux") + lax.axis_index("aux")
    small = table_copies(pairs, ranks, pairs_s, ranks_s, small_sems)
    small.append(pltpu.make_async_copy(counts, counts_s, small_sems.at[2]))
    small.append(pltpu.make_async_copy(amps.at[0:EARLY], amps_v, small_sems.at[3]))
    copies = [pltpu.make_async_copy(panels.at[o], raw.at[o], sems.at[o]) for o in range(orbitals)]
    for copy in small + copies:
        copy.start()
    for copy in small:
        copy.wait()
    live = counts_s[shard]
    for o in range(orbitals):
        copies[o].wait()

        def widen(t, carry):
            for side in range(2):
                slot = 2 * t + side
                slab = raw[o, slot]
                slab = jnp.where(slot < live, slab, jnp.zeros_like(slab))
                paired[o, t, side] = jnp.pad(slab, ((0, SLAB - width), (0, SLAB - width)))
            return carry

        lax.fori_loop(0, slots // 2, widen, 0, unroll=2)
    work = [(block * owned + p, amps_v[p], stored(out, p)) for p in range(EARLY)]
    terms(work, paired, squares, pairs_s, ranks_s)


def own_body(pairs, ranks, amps, paired, after, out, squares, pairs_s, ranks_s, sems):
    del after
    owned = amps.shape[0]
    small = table_copies(pairs, ranks, pairs_s, ranks_s, sems)
    for copy in small:
        copy.start()
    for copy in small:
        copy.wait()
    block = lax.axis_index("blk")
    work = [(block * owned + p, amps[p], stored(out, p - EARLY)) for p in range(EARLY, owned)]
    terms(work, paired, squares, pairs_s, ranks_s)


def other_body(pairs, ranks, near, far, paired, near_out, far_out, squares, pairs_s, ranks_s, sems):
    owned = near.shape[0]
    blocks = lax.axis_size("blk")
    block = lax.axis_index("blk")
    small = table_copies(pairs, ranks, pairs_s, ranks_s, sems)
    for copy in small:
        copy.start()
    for copy in small:
        copy.wait()
    work = []
    for amps, out, hops in ((far, far_out, 2), (near, near_out, 1)):
        start = (block + hops) % blocks * owned
        work += [(start + p, amps[p], stored(out, p)) for p in range(owned)]
    terms(work, paired, squares, pairs_s, ranks_s)


def in_vmem():
    return pl.BlockSpec(memory_space=pltpu.VMEM)


def in_place():
    return pl.BlockSpec(memory_space=pltpu.HBM)


def kept_in_hbm(value):
    return pltpu.with_memory_space_constraint(value, pltpu.HBM)


def cost(pairs):
    return pl.CostEstimate(flops=pairs * 10**9, bytes_accessed=5 * 10**6, transcendentals=0)


def halves(count, width, kind):
    return jax.ShapeDtypeStruct((2, count, width // 2, width), kind)


def loaded(counts, pairs, ranks, amps, panels):
    orbitals, slots, width, _ = panels.shape
    return pl.pallas_call(
        load_body,
        out_shape=(
            pltpu.VMEM((orbitals, slots // 2, 2, SLAB, SLAB), BF16),
            halves(EARLY, width, F32),
        ),
        in_specs=[in_place()] * 5,
        out_specs=(in_vmem(), in_vmem()),
        scratch_shapes=[
            pltpu.VMEM(panels.shape, BF16),
            pltpu.VMEM((EARLY, width, width), BF16),
            pltpu.VMEM((EARLY, SLAB, SLAB), BF16),
            pltpu.SMEM(counts.shape, jnp.int32),
            pltpu.SMEM(pairs.shape, jnp.int32),
            pltpu.SMEM(ranks.shape, jnp.int32),
            pltpu.SemaphoreType.DMA((orbitals,)),
            pltpu.SemaphoreType.DMA((4,)),
        ],
        cost_estimate=cost(3),
        compiler_params=pltpu.CompilerParams(vmem_limit_bytes=16 * 2**20),
        name="loaded",
    )(counts, pairs, ranks, amps, panels)


def table_scratch(count, pairs, ranks):
    return [
        pltpu.VMEM((count, SLAB, SLAB), BF16),
        pltpu.SMEM(pairs.shape, jnp.int32),
        pltpu.SMEM(ranks.shape, jnp.int32),
        pltpu.SemaphoreType.DMA((2,)),
    ]


def own_terms(pairs, ranks, amps, paired, after):
    owned, width, _ = amps.shape
    return pl.pallas_call(
        own_body,
        out_shape=halves(owned - EARLY, width, F32),
        in_specs=[in_place(), in_place(), in_vmem(), in_vmem(), pl.BlockSpec(memory_space=pl.ANY)],
        out_specs=in_vmem(),
        scratch_shapes=table_scratch(owned - EARLY, pairs, ranks),
        cost_estimate=cost(2 * owned),
        compiler_params=pltpu.CompilerParams(vmem_limit_bytes=8 * 2**20),
        name="own_terms",
    )(pairs, ranks, amps, paired, after)


def other_terms(pairs, ranks, near, far, paired):
    owned, width, _ = near.shape
    return pl.pallas_call(
        other_body,
        out_shape=(halves(owned, width, BF16), halves(owned, width, BF16)),
        in_specs=[in_place(), in_place(), in_vmem(), in_vmem(), in_vmem()],
        out_specs=(in_vmem(), in_vmem()),
        scratch_shapes=table_scratch(2 * owned, pairs, ranks),
        cost_estimate=cost(2 * owned),
        compiler_params=pltpu.CompilerParams(vmem_limit_bytes=8 * 2**20),
        name="other_terms",
    )(pairs, ranks, near, far, paired)


def passed_along(value, axis, steps):
    count = lax.axis_size(axis)
    return lax.ppermute(value, axis, [(source, (source + steps) % count) for source in range(count)])


def shards(panels, aux_counts, pair_list, pair_ranks, amplitudes):
    side = lax.axis_index("aux")
    pairs = kept_in_hbm(pair_list.T)
    ranks = kept_in_hbm(pair_ranks)
    far_amps = passed_along(amplitudes, "blk", -2)
    near_amps = passed_along(amplitudes, "blk", -1)
    paired, early = loaded(kept_in_hbm(aux_counts), pairs, ranks, kept_in_hbm(amplitudes), kept_in_hbm(panels))
    near, far = other_terms(pairs, ranks, near_amps, far_amps, paired)
    late = own_terms(pairs, ranks, amplitudes, paired, far)
    far = passed_along(far, "blk", 2)
    near = passed_along(near, "blk", 1)

    def half(value, which):
        return lax.dynamic_index_in_dim(value, which, 0, keepdims=False).astype(F32)

    def summed(which):
        own = jnp.concatenate([half(early, which), half(late, which)], axis=0)
        return own + half(near, which) + half(far, which)

    received = passed_along(summed(1 - side).astype(BF16), "aux", 1)
    return summed(side) + received.astype(F32)


def solution(mesh):
    placed = (P(None, ("blk", "aux"), None, None), P(), P(), P(), P("blk", None, None))
    return jax.shard_map(
        shards, mesh=mesh, in_specs=placed, out_specs=P("blk", "aux", None), check_vma=False
    )
```

```python
import functools
import jax
import jax.numpy as jnp
from jax import lax
from jax.experimental import pallas as pl
from jax.experimental.pallas import tpu as pltpu
from jax.sharding import PartitionSpec as P

F32, BF16 = jnp.float32, jnp.bfloat16
SLAB = 128
STEP = 2
EARLY = 2


def table_copies(pairs, ranks, pairs_s, ranks_s, sems):
    return [
        pltpu.make_async_copy(pairs, pairs_s, sems.at[0]),
        pltpu.make_async_copy(ranks, ranks_s, sems.at[1]),
    ]


def slot_pair(paired, orbital, t):
    return jnp.concatenate([paired[orbital, t, 0], paired[orbital, t, 1]], axis=1)


def on_diagonal(square):
    empty = jnp.zeros_like(square)
    upper = jnp.concatenate([square, empty], axis=1)
    lower = jnp.concatenate([empty, square], axis=1)
    return jnp.concatenate([upper, lower], axis=0)


def terms(work, paired, squares, pairs_s, ranks_s):
    slot_pairs = paired.shape[1]
    prepared = []
    for n, (row, amps, put) in enumerate(work):
        width = amps.shape[0]
        rank = ranks_s[row]
        rows = lax.broadcasted_iota(jnp.int32, (width, width), 0)
        cols = lax.broadcasted_iota(jnp.int32, (width, width), 1)
        masked = jnp.where((rows < rank) & (cols < rank), amps, jnp.zeros_like(amps))
        squares[n] = jnp.pad(masked, ((0, SLAB - width), (0, SLAB - width)))
        prepared.append((pairs_s[0, row], pairs_s[1, row], rank, rows, cols, put))
    for n, (left, right, rank, rows, cols, put) in enumerate(prepared):
        width = rows.shape[0]
        total = jnp.zeros((SLAB, SLAB), F32)
        for first in range(0, slot_pairs, STEP):
            taken = range(first, min(first + STEP, slot_pairs))
            lhs = jnp.concatenate([slot_pair(paired, left, t) for t in taken], axis=0)
            half = jnp.dot(lhs, on_diagonal(squares[n]), preferred_element_type=F32)
            for k, t in enumerate(taken):
                part = half[k * SLAB : (k + 1) * SLAB].astype(BF16)
                total = total + lax.dot_general(
                    part, slot_pair(paired, right, t), (((1,), (1,)), ((), ())), preferred_element_type=F32
                )
        put(jnp.where((rows < rank) & (cols < rank), total[:width, :width], 0.0))


def stored(out, p):
    def put(value):
        cut = value.shape[0] // 2
        out[0, p] = value[:cut].astype(out.dtype)
        out[1, p] = value[cut:].astype(out.dtype)

    return put


def load_body(counts, pairs, ranks, amps, panels, paired, out, raw, amps_v, squares, counts_s, pairs_s, ranks_s, sems, small_sems):
    orbitals, slots, width, _ = panels.shape
    owned = amps.shape[0]
    block = lax.axis_index("blk")
    shard = block * lax.axis_size("aux") + lax.axis_index("aux")
    small = table_copies(pairs, ranks, pairs_s, ranks_s, small_sems)
    small.append(pltpu.make_async_copy(counts, counts_s, small_sems.at[2]))
    small.append(pltpu.make_async_copy(amps.at[0:EARLY], amps_v, small_sems.at[3]))
    copies = [pltpu.make_async_copy(panels.at[o], raw.at[o], sems.at[o]) for o in range(orbitals)]
    for copy in small + copies:
        copy.start()
    for copy in small:
        copy.wait()
    live = counts_s[shard]
    for o in range(orbitals):
        copies[o].wait()

        def widen(t, carry):
            for side in range(2):
                slot = 2 * t + side
                slab = raw[o, slot]
                slab = jnp.where(slot < live, slab, jnp.zeros_like(slab))
                paired[o, t, side] = jnp.pad(slab, ((0, SLAB - width), (0, SLAB - width)))
            return carry

        lax.fori_loop(0, slots // 2, widen, 0, unroll=2)
    work = [(block * owned + p, amps_v[p], stored(out, p)) for p in range(EARLY)]
    terms(work, paired, squares, pairs_s, ranks_s)


def group_body(first, hops, pairs, ranks, amps, paired, after, out, squares, pairs_s, ranks_s, sems):
    del after
    owned = amps.shape[0]
    small = table_copies(pairs, ranks, pairs_s, ranks_s, sems)
    for copy in small:
        copy.start()
    for copy in small:
        copy.wait()
    start = (lax.axis_index("blk") + hops) % lax.axis_size("blk") * owned
    work = [(start + p, amps[p], stored(out, p - first)) for p in range(first, owned)]
    terms(work, paired, squares, pairs_s, ranks_s)


def in_vmem():
    return pl.BlockSpec(memory_space=pltpu.VMEM)


def in_place():
    return pl.BlockSpec(memory_space=pltpu.HBM)


def kept_in_hbm(value):
    return pltpu.with_memory_space_constraint(value, pltpu.HBM)


def cost(pairs):
    return pl.CostEstimate(flops=pairs * 10**9, bytes_accessed=5 * 10**6, transcendentals=0)


def halves(count, width, kind):
    return jax.ShapeDtypeStruct((2, count, width // 2, width), kind)


def loaded(counts, pairs, ranks, amps, panels):
    orbitals, slots, width, _ = panels.shape
    return pl.pallas_call(
        load_body,
        out_shape=(
            pltpu.VMEM((orbitals, slots // 2, 2, SLAB, SLAB), BF16),
            halves(EARLY, width, F32),
        ),
        in_specs=[in_place()] * 5,
        out_specs=(in_vmem(), in_vmem()),
        scratch_shapes=[
            pltpu.VMEM(panels.shape, BF16),
            pltpu.VMEM((EARLY, width, width), BF16),
            pltpu.VMEM((EARLY, SLAB, SLAB), BF16),
            pltpu.SMEM(counts.shape, jnp.int32),
            pltpu.SMEM(pairs.shape, jnp.int32),
            pltpu.SMEM(ranks.shape, jnp.int32),
            pltpu.SemaphoreType.DMA((orbitals,)),
            pltpu.SemaphoreType.DMA((4,)),
        ],
        cost_estimate=cost(3),
        compiler_params=pltpu.CompilerParams(vmem_limit_bytes=16 * 2**20),
        name="loaded",
    )(counts, pairs, ranks, amps, panels)


def table_scratch(count, pairs, ranks):
    return [
        pltpu.VMEM((count, SLAB, SLAB), BF16),
        pltpu.SMEM(pairs.shape, jnp.int32),
        pltpu.SMEM(ranks.shape, jnp.int32),
        pltpu.SemaphoreType.DMA((2,)),
    ]


def group_terms(first, hops, kind, pairs, ranks, amps, paired, after):
    owned, width, _ = amps.shape
    anywhere = pl.BlockSpec(memory_space=pl.ANY)
    return pl.pallas_call(
        functools.partial(group_body, first, hops),
        out_shape=halves(owned - first, width, kind),
        in_specs=[anywhere, anywhere, in_vmem(), in_vmem(), anywhere],
        out_specs=in_vmem(),
        scratch_shapes=table_scratch(owned - first, pairs, ranks),
        cost_estimate=cost(owned - first),
        compiler_params=pltpu.CompilerParams(vmem_limit_bytes=8 * 2**20),
    )(pairs, ranks, amps, paired, after)


def passed_along(value, axis, steps):
    count = lax.axis_size(axis)
    return lax.ppermute(value, axis, [(source, (source + steps) % count) for source in range(count)])


def shards(panels, aux_counts, pair_list, pair_ranks, amplitudes):
    side = lax.axis_index("aux")
    pairs = pair_list.T
    ranks = pair_ranks
    far_amps = passed_along(amplitudes, "blk", -2)
    near_amps = passed_along(amplitudes, "blk", -1)
    paired, early = loaded(
        kept_in_hbm(aux_counts), kept_in_hbm(pairs), kept_in_hbm(ranks), kept_in_hbm(amplitudes), kept_in_hbm(panels)
    )
    far = group_terms(0, 2, BF16, pairs, ranks, far_amps, paired, early)
    near = group_terms(0, 1, BF16, pairs, ranks, near_amps, paired, far)
    late = group_terms(EARLY, 0, F32, pairs, ranks, amplitudes, paired, near)
    far = passed_along(far, "blk", 2)
    near = passed_along(near, "blk", 1)

    def half(value, which):
        return lax.dynamic_index_in_dim(value, which, 0, keepdims=False).astype(F32)

    def summed(which):
        own = jnp.concatenate([half(early, which), half(late, which)], axis=0)
        return own + half(near, which) + half(far, which)

    received = passed_along(summed(1 - side).astype(BF16), "aux", 1)
    return summed(side) + received.astype(F32)


def solution(mesh):
    placed = (P(None, ("blk", "aux"), None, None), P(), P(), P(), P("blk", None, None))
    return jax.shard_map(
        shards, mesh=mesh, in_specs=placed, out_specs=P("blk", "aux", None), check_vma=False
    )
```

```python
import functools
import jax
import jax.numpy as jnp
from jax import lax
from jax.experimental import pallas as pl
from jax.experimental.pallas import tpu as pltpu
from jax.sharding import PartitionSpec as P

F32, BF16 = jnp.float32, jnp.bfloat16
SLAB = 128
STEP = 2
EARLY = 1


def table_copies(pairs, ranks, pairs_s, ranks_s, sems):
    return [
        pltpu.make_async_copy(pairs, pairs_s, sems.at[0]),
        pltpu.make_async_copy(ranks, ranks_s, sems.at[1]),
    ]


def slot_pair(paired, orbital, t):
    return jnp.concatenate([paired[orbital, t, 0], paired[orbital, t, 1]], axis=1)


def on_diagonal(square):
    empty = jnp.zeros_like(square)
    upper = jnp.concatenate([square, empty], axis=1)
    lower = jnp.concatenate([empty, square], axis=1)
    return jnp.concatenate([upper, lower], axis=0)


def terms(work, paired, squares, pairs_s, ranks_s):
    slot_pairs = paired.shape[1]
    prepared = []
    for n, (row, amps, put) in enumerate(work):
        width = amps.shape[0]
        rank = ranks_s[row]
        rows = lax.broadcasted_iota(jnp.int32, (width, width), 0)
        cols = lax.broadcasted_iota(jnp.int32, (width, width), 1)
        masked = jnp.where((rows < rank) & (cols < rank), amps, jnp.zeros_like(amps))
        squares[n] = jnp.pad(masked, ((0, SLAB - width), (0, SLAB - width)))
        prepared.append((pairs_s[0, row], pairs_s[1, row], rank, rows, cols, put))
    for n, (left, right, rank, rows, cols, put) in enumerate(prepared):
        width = rows.shape[0]
        total = jnp.zeros((SLAB, SLAB), F32)
        for first in range(0, slot_pairs, STEP):
            taken = range(first, min(first + STEP, slot_pairs))
            lhs = jnp.concatenate([slot_pair(paired, left, t) for t in taken], axis=0)
            half = jnp.dot(lhs, on_diagonal(squares[n]), preferred_element_type=F32)
            for k, t in enumerate(taken):
                part = half[k * SLAB : (k + 1) * SLAB].astype(BF16)
                total = total + lax.dot_general(
                    part, slot_pair(paired, right, t), (((1,), (1,)), ((), ())), preferred_element_type=F32
                )
        put(jnp.where((rows < rank) & (cols < rank), total[:width, :width], 0.0))


def stored(out, p):
    lower = lax.axis_index("aux")

    def put(value):
        cut = value.shape[0] // 2
        out[lower, p] = value[:cut].astype(out.dtype)
        out[1 - lower, p] = value[cut:].astype(out.dtype)

    return put


def load_body(counts, pairs, ranks, amps, panels, paired, out, raw, amps_v, squares, counts_s, pairs_s, ranks_s, sems, small_sems):
    orbitals, slots, width, _ = panels.shape
    owned = amps.shape[0]
    block = lax.axis_index("blk")
    shard = block * lax.axis_size("aux") + lax.axis_index("aux")
    small = table_copies(pairs, ranks, pairs_s, ranks_s, small_sems)
    small.append(pltpu.make_async_copy(counts, counts_s, small_sems.at[2]))
    small.append(pltpu.make_async_copy(amps.at[0:EARLY], amps_v, small_sems.at[3]))
    copies = [pltpu.make_async_copy(panels.at[o], raw.at[o], sems.at[o]) for o in range(orbitals)]
    for copy in small + copies:
        copy.start()
    for copy in small:
        copy.wait()
    live = counts_s[shard]
    for o in range(orbitals):
        copies[o].wait()

        def widen(t, carry):
            for side in range(2):
                slot = 2 * t + side
                slab = raw[o, slot]
                slab = jnp.where(slot < live, slab, jnp.zeros_like(slab))
                paired[o, t, side] = jnp.pad(slab, ((0, SLAB - width), (0, SLAB - width)))
            return carry

        lax.fori_loop(0, slots // 2, widen, 0, unroll=2)
    work = [(block * owned + p, amps_v[p], stored(out, p)) for p in range(EARLY)]
    terms(work, paired, squares, pairs_s, ranks_s)


def group_body(first, hops, pairs, ranks, amps, paired, after, out, squares, pairs_s, ranks_s, sems):
    del after
    owned = amps.shape[0]
    small = table_copies(pairs, ranks, pairs_s, ranks_s, sems)
    for copy in small:
        copy.start()
    for copy in small:
        copy.wait()
    start = (lax.axis_index("blk") + hops) % lax.axis_size("blk") * owned
    work = [(start + p, amps[p], stored(out, p - first)) for p in range(first, owned)]
    terms(work, paired, squares, pairs_s, ranks_s)


def in_vmem():
    return pl.BlockSpec(memory_space=pltpu.VMEM)


def in_place():
    return pl.BlockSpec(memory_space=pltpu.HBM)


def kept_in_hbm(value):
    return pltpu.with_memory_space_constraint(value, pltpu.HBM)


def cost(pairs):
    return pl.CostEstimate(flops=pairs * 10**9, bytes_accessed=5 * 10**6, transcendentals=0)


def halves(count, width, kind):
    return jax.ShapeDtypeStruct((2, count, width // 2, width), kind)


def loaded(counts, pairs, ranks, amps, panels):
    orbitals, slots, width, _ = panels.shape
    return pl.pallas_call(
        load_body,
        out_shape=(
            pltpu.VMEM((orbitals, slots // 2, 2, SLAB, SLAB), BF16),
            halves(EARLY, width, F32),
        ),
        in_specs=[in_place()] * 5,
        out_specs=(in_vmem(), in_vmem()),
        scratch_shapes=[
            pltpu.VMEM(panels.shape, BF16),
            pltpu.VMEM((EARLY, width, width), BF16),
            pltpu.VMEM((EARLY, SLAB, SLAB), BF16),
            pltpu.SMEM(counts.shape, jnp.int32),
            pltpu.SMEM(pairs.shape, jnp.int32),
            pltpu.SMEM(ranks.shape, jnp.int32),
            pltpu.SemaphoreType.DMA((orbitals,)),
            pltpu.SemaphoreType.DMA((4,)),
        ],
        cost_estimate=cost(3),
        compiler_params=pltpu.CompilerParams(vmem_limit_bytes=16 * 2**20),
        name="loaded",
    )(counts, pairs, ranks, amps, panels)


def table_scratch(count, pairs, ranks):
    return [
        pltpu.VMEM((count, SLAB, SLAB), BF16),
        pltpu.SMEM(pairs.shape, jnp.int32),
        pltpu.SMEM(ranks.shape, jnp.int32),
        pltpu.SemaphoreType.DMA((2,)),
    ]


def group_terms(first, hops, kind, pairs, ranks, amps, paired, after):
    owned, width, _ = amps.shape
    anywhere = pl.BlockSpec(memory_space=pl.ANY)
    return pl.pallas_call(
        functools.partial(group_body, first, hops),
        out_shape=halves(owned - first, width, kind),
        in_specs=[anywhere, anywhere, in_vmem(), in_vmem(), anywhere],
        out_specs=in_vmem(),
        scratch_shapes=table_scratch(owned - first, pairs, ranks),
        cost_estimate=cost(owned - first),
        compiler_params=pltpu.CompilerParams(vmem_limit_bytes=8 * 2**20),
    )(pairs, ranks, amps, paired, after)


def passed_along(value, axis, steps):
    count = lax.axis_size(axis)
    return lax.ppermute(value, axis, [(source, (source + steps) % count) for source in range(count)])


def passed_across(value, steps):
    blocks = lax.axis_size("blk")
    route = [
        (2 * block + side, 2 * ((block + steps) % blocks) + 1 - side) for block in range(blocks) for side in range(2)
    ]
    return lax.ppermute(value, ("blk", "aux"), route)


def shards(panels, aux_counts, pair_list, pair_ranks, amplitudes):
    pairs = pair_list.T
    ranks = pair_ranks
    far_amps = passed_along(amplitudes, "blk", -2)
    near_amps = passed_along(amplitudes, "blk", -1)
    paired, early = loaded(
        kept_in_hbm(aux_counts), kept_in_hbm(pairs), kept_in_hbm(ranks), kept_in_hbm(amplitudes), kept_in_hbm(panels)
    )
    far = group_terms(0, 2, BF16, pairs, ranks, far_amps, paired, early)
    near = group_terms(0, 1, BF16, pairs, ranks, near_amps, paired, far)
    late = group_terms(EARLY, 0, F32, pairs, ranks, amplitudes, paired, near)
    far_same = passed_along(far[0], "blk", 2)
    far_other = passed_across(far[1], 2)
    near_same = passed_along(near[0], "blk", 1)
    near_other = passed_across(near[1], 1)
    own = jnp.concatenate([early[0], late[0]], axis=0)
    own_other = passed_across(jnp.concatenate([early[1], late[1]], axis=0).astype(BF16), 0)
    total = own
    for part in (far_same, far_other, near_same, near_other, own_other):
        total = total + part.astype(F32)
    return total


def solution(mesh):
    placed = (P(None, ("blk", "aux"), None, None), P(), P(), P(), P("blk", None, None))
    return jax.shard_map(
        shards, mesh=mesh, in_specs=placed, out_specs=P("blk", "aux", None), check_vma=False
    )
```

```python
import functools
import jax
import jax.numpy as jnp
from jax import lax
from jax.experimental import pallas as pl
from jax.experimental.pallas import tpu as pltpu
from jax.sharding import PartitionSpec as P

F32, BF16 = jnp.float32, jnp.bfloat16
SLAB = 128
STEP = 2


def table_copies(pairs, ranks, pairs_s, ranks_s, sems):
    return [
        pltpu.make_async_copy(pairs, pairs_s, sems.at[0]),
        pltpu.make_async_copy(ranks, ranks_s, sems.at[1]),
    ]


def slot_pair(paired, orbital, t):
    return jnp.concatenate([paired[orbital, t, 0], paired[orbital, t, 1]], axis=1)


def on_diagonal(square):
    empty = jnp.zeros_like(square)
    upper = jnp.concatenate([square, empty], axis=1)
    lower = jnp.concatenate([empty, square], axis=1)
    return jnp.concatenate([upper, lower], axis=0)


def terms(work, paired, squares, pairs_s, ranks_s):
    slot_pairs = paired.shape[1]
    prepared = []
    for n, (row, amps, put) in enumerate(work):
        width = amps.shape[0]
        rank = ranks_s[row]
        rows = lax.broadcasted_iota(jnp.int32, (width, width), 0)
        cols = lax.broadcasted_iota(jnp.int32, (width, width), 1)
        masked = jnp.where((rows < rank) & (cols < rank), amps, jnp.zeros_like(amps))
        squares[n] = jnp.pad(masked, ((0, SLAB - width), (0, SLAB - width)))
        prepared.append((pairs_s[0, row], pairs_s[1, row], rank, rows, cols, put))
    for n, (left, right, rank, rows, cols, put) in enumerate(prepared):
        width = rows.shape[0]
        total = jnp.zeros((SLAB, SLAB), F32)
        for first in range(0, slot_pairs, STEP):
            taken = range(first, min(first + STEP, slot_pairs))
            lhs = jnp.concatenate([slot_pair(paired, left, t) for t in taken], axis=0)
            half = jnp.dot(lhs, on_diagonal(squares[n]), preferred_element_type=F32)
            for k, t in enumerate(taken):
                part = half[k * SLAB : (k + 1) * SLAB].astype(BF16)
                total = total + lax.dot_general(
                    part, slot_pair(paired, right, t), (((1,), (1,)), ((), ())), preferred_element_type=F32
                )
        put(jnp.where((rows < rank) & (cols < rank), total[:width, :width], 0.0))


def stored(out, p):
    lower = lax.axis_index("aux")

    def put(value):
        cut = value.shape[0] // 2
        out[lower, p] = value[:cut].astype(out.dtype)
        out[1 - lower, p] = value[cut:].astype(out.dtype)

    return put


def load_body(counts, pairs, ranks, amps, panels, paired, out, raw, amps_v, squares, counts_s, pairs_s, ranks_s, sems, small_sems):
    orbitals, slots, width, _ = panels.shape
    owned = amps.shape[0]
    block = lax.axis_index("blk")
    shard = block * lax.axis_size("aux") + lax.axis_index("aux")
    small = table_copies(pairs, ranks, pairs_s, ranks_s, small_sems)
    small.append(pltpu.make_async_copy(counts, counts_s, small_sems.at[2]))
    small.append(pltpu.make_async_copy(amps, amps_v, small_sems.at[3]))
    copies = [pltpu.make_async_copy(panels.at[o], raw.at[o], sems.at[o]) for o in range(orbitals)]
    for copy in small + copies:
        copy.start()
    for copy in small:
        copy.wait()
    live = counts_s[shard]
    for o in range(orbitals):
        copies[o].wait()

        def widen(t, carry):
            for side in range(2):
                slot = 2 * t + side
                slab = raw[o, slot]
                slab = jnp.where(slot < live, slab, jnp.zeros_like(slab))
                paired[o, t, side] = jnp.pad(slab, ((0, SLAB - width), (0, SLAB - width)))
            return carry

        lax.fori_loop(0, slots // 2, widen, 0, unroll=2)
    work = [(block * owned + p, amps_v[p], stored(out, p)) for p in range(owned)]
    terms(work, paired, squares, pairs_s, ranks_s)


def group_body(first, hops, pairs, ranks, amps, paired, after, out, squares, pairs_s, ranks_s, sems):
    del after
    owned = amps.shape[0]
    small = table_copies(pairs, ranks, pairs_s, ranks_s, sems)
    for copy in small:
        copy.start()
    for copy in small:
        copy.wait()
    start = (lax.axis_index("blk") + hops) % lax.axis_size("blk") * owned
    work = [(start + p, amps[p], stored(out, p - first)) for p in range(first, owned)]
    terms(work, paired, squares, pairs_s, ranks_s)


def in_vmem():
    return pl.BlockSpec(memory_space=pltpu.VMEM)


def in_place():
    return pl.BlockSpec(memory_space=pltpu.HBM)


def kept_in_hbm(value):
    return pltpu.with_memory_space_constraint(value, pltpu.HBM)


def cost(pairs):
    return pl.CostEstimate(flops=pairs * 10**9, bytes_accessed=5 * 10**6, transcendentals=0)


def halves(count, width, kind):
    return jax.ShapeDtypeStruct((2, count, width // 2, width), kind)


def loaded(counts, pairs, ranks, amps, panels):
    orbitals, slots, width, _ = panels.shape
    owned = amps.shape[0]
    return pl.pallas_call(
        load_body,
        out_shape=(
            pltpu.VMEM((orbitals, slots // 2, 2, SLAB, SLAB), BF16),
            halves(owned, width, F32),
        ),
        in_specs=[in_place()] * 5,
        out_specs=(in_vmem(), in_vmem()),
        scratch_shapes=[
            pltpu.VMEM(panels.shape, BF16),
            pltpu.VMEM(amps.shape, BF16),
            pltpu.VMEM((owned, SLAB, SLAB), BF16),
            pltpu.SMEM(counts.shape, jnp.int32),
            pltpu.SMEM(pairs.shape, jnp.int32),
            pltpu.SMEM(ranks.shape, jnp.int32),
            pltpu.SemaphoreType.DMA((orbitals,)),
            pltpu.SemaphoreType.DMA((4,)),
        ],
        cost_estimate=cost(3),
        compiler_params=pltpu.CompilerParams(vmem_limit_bytes=16 * 2**20),
        name="loaded",
    )(counts, pairs, ranks, amps, panels)


def table_scratch(count, pairs, ranks):
    return [
        pltpu.VMEM((count, SLAB, SLAB), BF16),
        pltpu.SMEM(pairs.shape, jnp.int32),
        pltpu.SMEM(ranks.shape, jnp.int32),
        pltpu.SemaphoreType.DMA((2,)),
    ]


def group_terms(first, hops, kind, pairs, ranks, amps, paired, after):
    owned, width, _ = amps.shape
    anywhere = pl.BlockSpec(memory_space=pl.ANY)
    return pl.pallas_call(
        functools.partial(group_body, first, hops),
        out_shape=halves(owned - first, width, kind),
        in_specs=[anywhere, anywhere, in_vmem(), in_vmem(), anywhere],
        out_specs=in_vmem(),
        scratch_shapes=table_scratch(owned - first, pairs, ranks),
        cost_estimate=cost(owned - first),
        compiler_params=pltpu.CompilerParams(vmem_limit_bytes=8 * 2**20),
    )(pairs, ranks, amps, paired, after)


def passed_along(value, axis, steps):
    count = lax.axis_size(axis)
    return lax.ppermute(value, axis, [(source, (source + steps) % count) for source in range(count)])


def passed_across(value, steps):
    blocks = lax.axis_size("blk")
    route = [
        (2 * block + side, 2 * ((block + steps) % blocks) + 1 - side) for block in range(blocks) for side in range(2)
    ]
    return lax.ppermute(value, ("blk", "aux"), route)


def shards(panels, aux_counts, pair_list, pair_ranks, amplitudes):
    pairs = pair_list.T
    ranks = pair_ranks
    far_amps = passed_along(amplitudes, "blk", -2)
    near_amps = passed_along(amplitudes, "blk", -1)
    paired, own = loaded(
        kept_in_hbm(aux_counts), kept_in_hbm(pairs), kept_in_hbm(ranks), kept_in_hbm(amplitudes), kept_in_hbm(panels)
    )
    own_other = passed_across(own[1].astype(BF16), 0)
    far = group_terms(0, 2, BF16, pairs, ranks, far_amps, paired, own)
    near = group_terms(0, 1, BF16, pairs, ranks, near_amps, paired, far)
    far_other = passed_across(far[1], 2)
    far_same = passed_along(far[0], "blk", 2)
    near_other = passed_across(near[1], 1)
    near_same = passed_along(near[0], "blk", 1)
    total = own[0]
    for part in (own_other, far_same, far_other, near_same, near_other):
        total = total + part.astype(F32)
    return total


def solution(mesh):
    placed = (P(None, ("blk", "aux"), None, None), P(), P(), P(), P("blk", None, None))
    return jax.shard_map(
        shards, mesh=mesh, in_specs=placed, out_specs=P("blk", "aux", None), check_vma=False
    )
```
